32 devices in a mesh: gx: 4 (over y, core), gy: 8 (over z, x).
Axes of the slice: x: 2, y: 2, z: 4, core: 2. Of those that a mesh axis runs over, the one named last changes fastest.
Arguments:
- pool_old: float32 [40, 131072], P(None, ('gx', 'gy')), may hold values from 0.5 to 2
- pool_new: float32 [40, 131072], P(None, ('gx', 'gy')), may hold values from 0.5 to 2
- flux: float32 [40, 131072], P(None, ('gx', 'gy')), may hold values from -6 to 6
- area: float32 [131072], P(('gx', 'gy')), may hold values from 0.05 to 1
- pft_id: int32 [131072], P(('gx', 'gy')), may hold values from 0 to 78
- region_id: int32 [131072], P(('gx', 'gy')), may hold values from 0 to 31, as said below
Outputs:
- pool_totals: float32 [40, 2528], replicated
- error_totals: float32 [40, 2528], replicated
The draws below stay inside these ranges and needn't reach their ends.
Inputs may be any that keep to these rules, and one draw needn't show every extreme that they name: `region_id`: patch i lies in block k = i // 4096; with K = 32 blocks, its region is (k * 32) // K or ((k * 32) // K + 1) mod 32.
All inputs are finite; a program needn't handle non-finite values.
Results may differ from the reference program's by a relative error of at most 0.000076.
Values sent between devices are 32-bit elements; how exact they have to be, the bound alone decides.
A program may use at most 64 MiB of HBM per device.

```python
import math
import jax
import jax.numpy as jnp
import numpy as np

POOLS = 40
PFT = 79
REGION = 32
PATCH_DEV = 4096
CELLS = 2528
PATCHES = 131072
DEVICES = 32


def draw_region_id(key, part):
    index = jnp.arange(PATCHES, dtype=jnp.int32)
    block = index // PATCH_DEV
    base = block * REGION // DEVICES
    picks = jax.random.randint(key, (PATCHES,), 0, 4)
    region = jnp.where(picks == 0, base + 1, base) % REGION
    return region.astype(jnp.int32)


def plant(values, key, low, high):
    spot = [jax.random.randint(jax.random.fold_in(key, axis), (), 0, length) for axis, length in enumerate(values.shape)]
    widest = values.shape.index(max(values.shape))
    neighbour = spot[:widest] + [(spot[widest] + 1) % values.shape[widest]] + spot[widest + 1:]
    return values.at[tuple(spot)].set(low).at[tuple(neighbour)].set(high)


def block_levels(rng, extent, split, least, top_value):
    loudness, own = 1.0, jax.random.fold_in(rng, 6)
    for axis_at, blocks in split:
        steps = jnp.exp(jax.random.uniform(jax.random.fold_in(own, axis_at), (blocks,), jnp.float32, least / len(split), top_value / len(split)))
        loudness = loudness * jnp.repeat(steps, extent[axis_at] // blocks).reshape([-1 if axis == axis_at else 1 for axis in range(len(extent))])
    return loudness


def rank_bounds(amount, skew):
    loads = [(1 << 20) // math.isqrt(rank ** skew) + 1 for rank in range(1, amount + 1)]
    width = 1 + sum(loads) // (1 << 30)
    return np.cumsum(np.array([max(1, weight // width) for weight in loads]))


def ranked(stream_key, extent, amount, skew):
    listing = rank_bounds(amount, skew)
    ticket = jax.random.randint(jax.random.fold_in(stream_key, 1), extent, 0, int(listing[amount - 1]))
    standing = jnp.searchsorted(jnp.asarray(listing, jnp.int32), ticket, side="right")
    return jax.random.permutation(jax.random.fold_in(stream_key, 2), amount)[standing].astype(jnp.int32)


def scatter_about(key, dims, deviation, most, split=(), held_as=jnp.bfloat16):
    entries = jax.random.normal(key, dims, jnp.float32) * deviation
    if len(split) > 0:
        entries = block_levels(key, dims, split, -0.22, 0.18) * entries
    return jnp.clip(entries, min=-most, max=most).astype(held_as)


def setup_inputs(seed: int = 0) -> dict:
    streams_of = jax.random.split(jax.random.key(seed), 7)
    pool_old = jnp.clip(0.5 + 1.5 * jax.random.uniform(streams_of[0], (POOLS, PATCHES), jnp.float32) ** block_levels(streams_of[0], (POOLS, PATCHES), ((1, 32),), -0.2, 0.2), 0.5, 2.0)
    pool_new = jnp.clip(0.5 + 1.5 * jax.random.uniform(streams_of[1], (POOLS, PATCHES), jnp.float32) ** block_levels(streams_of[1], (POOLS, PATCHES), ((1, 32),), -0.2, 0.2), 0.5, 2.0)
    flux = scatter_about(streams_of[2], (POOLS, PATCHES), 1.0, 6.0, ((1, 32),), jnp.float32)
    area = jnp.clip(jnp.exp(math.log(1.0) - 2.9957323 * jax.random.uniform(streams_of[3], (PATCHES,), jnp.float32) ** block_levels(streams_of[3], (PATCHES,), ((0, 32),), -0.2, 0.2)), 0.05, 1.0)
    pft_id = plant(ranked(streams_of[4], (PATCHES,), PFT, 2), jax.random.fold_in(streams_of[4], 3), 0, PFT - 1).astype(jnp.int32)
    region_id = draw_region_id(jax.random.fold_in(streams_of[6], 71), 0)
    return {"pool_old": pool_old, "pool_new": pool_new, "flux": flux, "area": area, "pft_id": pft_id, "region_id": region_id}


def reference(pool_old, pool_new, flux, area, pft_id, region_id):
    cell = (pft_id * REGION + region_id).astype(jnp.int32)
    stored = area[None, :] * pool_new
    balance = area[None, :] * (pool_new - pool_old - 0.5 * flux)
    stacked = jnp.concatenate([stored, balance], axis=0)
    totals = jax.ops.segment_sum(stacked.T, cell, num_segments=CELLS).T
    totals = totals * jnp.float32(CELLS / PATCHES)
    return (totals[:POOLS], totals[POOLS:])
```

```python
import functools
import jax
import jax.numpy as jnp
from jax import lax
from jax.experimental import pallas as pl
from jax.experimental.pallas import tpu as pltpu
from jax.sharding import PartitionSpec as P

POOLS = 40
PFT = 79
REGION = 32
CELLS = 2528
MESH = pl.DeviceIdType.MESH
ROWS = 2 * POOLS
PFT_PAD = 80
MAIN = 56
REST = PFT_PAD - MAIN
LANES = 128
SPARE = LANES - ROWS
BLOCKS = 4


def pack(table):
    main = table[:MAIN]
    rest = table[MAIN:]
    lane = lax.broadcasted_iota(jnp.int32, (REST, LANES), 1)
    first = pltpu.roll(rest, ROWS, 1)
    second = pltpu.roll(rest, ROWS - SPARE, 1)
    top = jnp.where(lane < ROWS, main[:REST], first)
    middle = jnp.where(lane < ROWS, main[REST : 2 * REST], second)
    return jnp.concatenate([top, middle, main[2 * REST :]], axis=0)


def kernel(
    zs, ys, scale,
    old_hbm, new_hbm, flux_hbm, area_ref, pft_ref, region_ref,
    stored_ref, error_ref,
    old_v, new_v, flux_v, nxt, halo, gathered,
    in_sem, halo_send, halo_recv, send_sem, recv_sem,
):
    gx, gy = lax.axis_index("gx"), lax.axis_index("gy")
    ny = 2 * zs
    devices = 2 * ys * ny
    patches = area_ref.shape[1]
    width = patches // BLOCKS
    y, c = gx // 2, gx % 2
    z, x = gy // 2, gy % 2
    me = gx * ny + gy
    copies = []
    for k in range(BLOCKS):
        part = pl.ds(k * width, width)
        for a, (src, dst) in enumerate(((new_hbm, new_v), (old_hbm, old_v), (flux_hbm, flux_v))):
            copy = pltpu.make_async_copy(src.at[:, part], dst.at[:, part], in_sem.at[a, k])
            copy.start()
            copies.append(copy)

    def dev(y_, c_, z_, x_):
        return (y_ * 2 + c_, z_ * 2 + x_)

    def slot(y_, c_, z_, x_):
        return (y_ * 2 + c_) * ny + z_ * 2 + x_

    after = lax.rem(me + 1, devices)
    before = lax.rem(me + devices - 1, devices)
    dev_after = (after // ny, lax.rem(after, ny))
    dev_before = (before // ny, lax.rem(before, ny))
    z_peers = [lax.rem(z + k, zs) for k in range(1, zs)]
    dev_x, dev_y, dev_c = dev(y, c, z, 1 - x), dev(1 - y, c, z, x), dev(y, 1 - c, z, x)
    partners = [dev(y, c, q, x) for q in z_peers] + [dev_x, dev_y, dev_c, dev_after, dev_before]
    barrier = pltpu.get_barrier_semaphore()
    for partner in partners:
        pl.semaphore_signal(barrier, inc=1, device_id=partner, device_id_type=MESH)

    base = me * REGION // devices
    total = None
    for k in range(BLOCKS):
        part = pl.ds(k * width, width)
        code = pft_ref[:, part] + jnp.where(region_ref[:, part] == base, 0, PFT_PAD)
        cells = lax.broadcasted_iota(jnp.int32, (2 * PFT_PAD, width), 0)
        hot = jnp.where(cells == code, 1.0, 0.0).astype(jnp.bfloat16)
        for copy in copies[3 * k : 3 * k + 3]:
            copy.wait()
        area = area_ref[:, part]
        new = new_v[:, part]
        stored = area * new
        balance = area * (new - old_v[:, part] - 0.5 * flux_v[:, part])
        values = jnp.concatenate([stored, balance], axis=0)
        high = values.astype(jnp.bfloat16)
        left = values - high.astype(jnp.float32)
        middle = left.astype(jnp.bfloat16)
        low = (left - middle.astype(jnp.float32)).astype(jnp.bfloat16)
        pieces = jnp.concatenate([high, middle, low], axis=0)
        added = lax.dot_general(hot, pieces, (((1,), (1,)), ((), ())), preferred_element_type=jnp.float32)
        total = added if total is None else total + added
    wide = jnp.concatenate([total, jnp.zeros((2 * PFT_PAD, 2 * LANES - 3 * ROWS), jnp.float32)], axis=1)
    first = wide[:, :LANES]
    second = wide[:, LANES:]
    lane = lax.broadcasted_iota(jnp.int32, (2 * PFT_PAD, LANES), 1)
    mid = jnp.where(lane < LANES - ROWS, pltpu.roll(first, LANES - ROWS, 1), pltpu.roll(second, LANES - ROWS, 1))
    last = pltpu.roll(second, 2 * LANES - 2 * ROWS, 1)
    table = (first + mid + last) * scale
    own = pack(table[:PFT_PAD])
    nxt[...] = pack(table[PFT_PAD:])

    pl.semaphore_wait(barrier, len(partners))
    halo_copy = pltpu.make_async_remote_copy(
        src_ref=nxt, dst_ref=halo, send_sem=halo_send, recv_sem=halo_recv,
        device_id=dev_after, device_id_type=MESH,
    )
    halo_copy.start()
    halo_copy.wait_recv()

    def chunk(s):
        return gathered.at[pl.ds(pl.multiple_of(s * MAIN, 8), MAIN), :]

    gathered[pl.ds(pl.multiple_of(me * MAIN, 8), MAIN), :] = own + halo[...]
    sent = []

    def send(s, target):
        copy = pltpu.make_async_remote_copy(
            src_ref=chunk(s), dst_ref=chunk(s), send_sem=send_sem.at[len(sent)],
            recv_sem=recv_sem.at[s], device_id=target, device_id_type=MESH,
        )
        copy.start()
        sent.append(copy)

    def arrive(s):
        pltpu.make_async_remote_copy(
            src_ref=chunk(s), dst_ref=chunk(s), send_sem=send_sem.at[0],
            recv_sem=recv_sem.at[s], device_id=dev_x, device_id_type=MESH,
        ).wait_recv()

    send(me, dev_y)
    send(me, dev_x)
    for q in z_peers:
        send(me, dev(y, c, q, x))
    send(me, dev_c)
    for q in z_peers:
        s = slot(y, c, q, x)
        arrive(s)
        send(s, dev_y)
        send(s, dev_x)
        send(s, dev_c)
    for k, q in enumerate([z] + z_peers):
        s = slot(y, c, q, 1 - x)
        arrive(s)
        if k % 2 == 0:
            send(s, dev_y)
        send(s, dev_c)
        s = slot(1 - y, c, q, x)
        arrive(s)
        if k % 2 == 1:
            send(s, dev_x)
        send(s, dev_c)
    for q in [z] + z_peers:
        s = slot(1 - y, c, q, 1 - x)
        arrive(s)
        send(s, dev_c)
    for q in [z] + z_peers:
        for y_, x_ in ((y, x), (y, 1 - x), (1 - y, x), (1 - y, 1 - x)):
            arrive(slot(y_, 1 - c, q, x_))
    halo_copy.wait_send()
    for copy in sent:
        copy.wait_send()

    for u in range(MAIN // 4):
        rows = [gathered[pl.ds(4 * u + j, REGION, stride=MAIN), :] for j in range(4)]
        tile = jnp.concatenate(rows, axis=0).T
        here = pl.ds(u * LANES, LANES)
        stored_ref[:, here] = tile[:POOLS]
        error_ref[:, here] = tile[POOLS:ROWS]
        if 4 * u < 2 * REST:
            t = (MAIN // 4) + (u if 4 * u < REST else u - REST // 4)
            w = min(LANES, CELLS - t * LANES)
            there = pl.ds(t * LANES, w)
            if 4 * u < REST:
                stored_ref[:, there] = tile[ROWS : ROWS + POOLS, :w]
                error_ref[: SPARE - POOLS, there] = tile[ROWS + POOLS :, :w]
            else:
                error_ref[SPARE - POOLS :, there] = tile[ROWS : 2 * ROWS - SPARE, :w]


def kernel_shards(zs, ys, pool_old, pool_new, flux, area, pft_id, region_id):
    patches = area.shape[0]
    devices = 4 * ys * zs
    scale = CELLS / (patches * devices)
    out = jax.ShapeDtypeStruct((POOLS, CELLS), jnp.float32)
    hbm, vmem = pl.BlockSpec(memory_space=pl.ANY), pl.BlockSpec(memory_space=pltpu.VMEM)
    sends = 3 + zs - 1 + 3 * (zs - 1) + 3 * zs + zs
    return pl.pallas_call(
        functools.partial(kernel, zs, ys, scale),
        out_shape=(out, out),
        in_specs=[hbm] * 3 + [vmem] * 3,
        out_specs=(vmem, vmem),
        scratch_shapes=[
            pltpu.VMEM((POOLS, patches), jnp.float32),
            pltpu.VMEM((POOLS, patches), jnp.float32),
            pltpu.VMEM((POOLS, patches), jnp.float32),
            pltpu.VMEM((MAIN, LANES), jnp.float32),
            pltpu.VMEM((MAIN, LANES), jnp.float32),
            pltpu.VMEM((REGION * MAIN, LANES), jnp.float32),
            pltpu.SemaphoreType.DMA((3, BLOCKS)),
            pltpu.SemaphoreType.DMA,
            pltpu.SemaphoreType.DMA,
            pltpu.SemaphoreType.DMA((sends,)),
            pltpu.SemaphoreType.DMA((devices,)),
        ],
        compiler_params=pltpu.CompilerParams(collective_id=0, has_side_effects=True),
    )(pool_old, pool_new, flux, area[None, :], pft_id[None, :], region_id[None, :])


def shards(pool_old, pool_new, flux, area, pft_id, region_id):
    width_x = lax.axis_size("gx")
    width_y = lax.axis_size("gy")
    devices_all = width_x * width_y
    position = lax.axis_index("gx") * width_y + lax.axis_index("gy")
    base = position * REGION // devices_all
    offset_here = (region_id - base) % REGION
    compact_cell = pft_id * 2 + offset_here
    stored = area[None, :] * pool_new
    balance = area[None, :] * (pool_new - pool_old - 0.5 * flux)
    stacked = jnp.concatenate([stored, balance], axis=0)
    rows = stacked.shape[0]
    patch_count = stacked.shape[1]
    block = min(512, patch_count)
    blocks = patch_count // block
    stacked_blocks = stacked.reshape(rows, blocks, block).transpose(1, 0, 2)
    cell_blocks = compact_cell.reshape(blocks, block)
    columns = jnp.arange(2 * PFT, dtype=jnp.int32)

    def accumulate(totals, inputs):
        values, cells_here = inputs
        onehot = (cells_here[:, None] == columns[None, :]).astype(jnp.float32)
        added = jnp.dot(
            values, onehot, preferred_element_type=jnp.float32, precision=lax.Precision.HIGHEST
        )
        return (totals + added, None)

    local_table, _ = lax.scan(
        accumulate, jnp.zeros((rows, 2 * PFT), jnp.float32), (stacked_blocks, cell_blocks)
    )
    local_table = local_table.reshape(rows, PFT, 2)
    region_axis = jnp.arange(REGION, dtype=jnp.int32)
    pair_axis = jnp.arange(2, dtype=jnp.int32)
    span = REGION // width_x + 1
    start = lax.axis_index("gx") * (REGION // width_x)
    span_axis = jnp.arange(span, dtype=jnp.int32)
    into_group = ((base - start + pair_axis)[:, None] == span_axis[None, :]).astype(jnp.float32)
    group_table = jnp.einsum(
        "apj,jw->apw", local_table, into_group, precision=lax.Precision.HIGHEST
    )
    group_total = lax.psum(group_table, "gy")
    into_full = (((start + span_axis) % REGION)[:, None] == region_axis[None, :]).astype(
        jnp.float32
    )
    placed = jnp.einsum("apw,wr->apr", group_total, into_full, precision=lax.Precision.HIGHEST)
    totals = lax.psum(placed.reshape(rows, CELLS), "gx")
    patch_all = patch_count * devices_all
    totals = totals * jnp.float32(CELLS / patch_all)
    return (totals[:POOLS], totals[POOLS:])


def solution(mesh):
    wide, deep = mesh.shape["gx"], mesh.shape["gy"]
    if wide == 4 and wide * deep == REGION:
        local = functools.partial(kernel_shards, deep // 2, wide // 2)
    else:
        local = shards
    return jax.shard_map(
        local,
        mesh=mesh,
        in_specs=(
            P(None, ("gx", "gy")),
            P(None, ("gx", "gy")),
            P(None, ("gx", "gy")),
            P(("gx", "gy")),
            P(("gx", "gy")),
            P(("gx", "gy")),
        ),
        out_specs=(P(), P()),
        check_vma=False,
    )
```

```python
import functools
import jax
import jax.numpy as jnp
from jax import lax
from jax.experimental import pallas as pl
from jax.experimental.pallas import tpu as pltpu
from jax.sharding import PartitionSpec as P

POOLS = 40
PFT = 79
REGION = 32
CELLS = 2528
MESH = pl.DeviceIdType.MESH
ROWS = 2 * POOLS
PFT_PAD = 80
MAIN = 56
REST = PFT_PAD - MAIN
LANES = 128
SPARE = LANES - ROWS
BLOCKS = 4


def pack(table):
    main = table[:MAIN]
    rest = table[MAIN:]
    lane = lax.broadcasted_iota(jnp.int32, (REST, LANES), 1)
    first = pltpu.roll(rest, ROWS, 1)
    second = pltpu.roll(rest, ROWS - SPARE, 1)
    top = jnp.where(lane < ROWS, main[:REST], first)
    middle = jnp.where(lane < ROWS, main[REST : 2 * REST], second)
    return jnp.concatenate([top, middle, main[2 * REST :]], axis=0)


def kernel(
    zs, ys, scale,
    old_hbm, new_hbm, flux_hbm, area_ref, pft_ref, region_ref,
    stored_ref, error_ref,
    old_v, new_v, flux_v, own, nxt, theirs, halo, gathered,
    in_sem, halo_send, halo_recv, send_sem, recv_sem,
):
    gx, gy = lax.axis_index("gx"), lax.axis_index("gy")
    ny = 2 * zs
    devices = 2 * ys * ny
    patches = area_ref.shape[1]
    width = patches // BLOCKS
    y, c = gx // 2, gx % 2
    z, x = gy // 2, gy % 2
    me = gx * ny + gy
    copies = []
    for k in range(BLOCKS):
        part = pl.ds(k * width, width)
        for a, (src, dst) in enumerate(((new_hbm, new_v), (old_hbm, old_v), (flux_hbm, flux_v))):
            copy = pltpu.make_async_copy(src.at[:, part], dst.at[:, part], in_sem.at[a, k])
            copy.start()
            copies.append(copy)

    def dev(y_, c_, z_, x_):
        return (y_ * 2 + c_, z_ * 2 + x_)

    def slot(y_, c_, z_, x_):
        return (y_ * 2 + c_) * ny + z_ * 2 + 1 - x_

    by_distance = [sorted(range(zs), key=lambda q, a=a: (abs(q - a), q)) for a in range(zs)]
    line = [sum(jnp.where(z == a, by_distance[a][k], 0) for a in range(zs)) for k in range(zs)]
    dev_x, dev_y, dev_c = dev(y, c, z, 1 - x), dev(1 - y, c, z, x), dev(y, 1 - c, z, x)
    dev_d = dev(1 - y, c, z, 1 - x)
    partners = [dev(y, c, q, x) for q in line[1:]] + [dev_x, dev_y, dev_d, dev_c]
    barrier = pltpu.get_barrier_semaphore()
    for partner in partners:
        pl.semaphore_signal(barrier, inc=1, device_id=partner, device_id_type=MESH)

    base = me * REGION // devices
    total = None
    for k in range(BLOCKS):
        part = pl.ds(k * width, width)
        code = pft_ref[:, part] + jnp.where(region_ref[:, part] == base, 0, PFT_PAD)
        cells = lax.broadcasted_iota(jnp.int32, (2 * PFT_PAD, width), 0)
        hot = jnp.where(cells == code, 1.0, 0.0).astype(jnp.bfloat16)
        for copy in copies[3 * k : 3 * k + 3]:
            copy.wait()
        area = area_ref[:, part]
        new = new_v[:, part]
        stored = area * new
        balance = area * (new - old_v[:, part] - 0.5 * flux_v[:, part])
        values = jnp.concatenate([stored, balance], axis=0)
        high = values.astype(jnp.bfloat16)
        left = values - high.astype(jnp.float32)
        middle = left.astype(jnp.bfloat16)
        low = (left - middle.astype(jnp.float32)).astype(jnp.bfloat16)
        pieces = jnp.concatenate([high, middle, low], axis=0)
        added = lax.dot_general(hot, pieces, (((1,), (1,)), ((), ())), preferred_element_type=jnp.float32)
        total = added if total is None else total + added
    wide = jnp.concatenate([total, jnp.zeros((2 * PFT_PAD, 2 * LANES - 3 * ROWS), jnp.float32)], axis=1)
    first = wide[:, :LANES]
    second = wide[:, LANES:]
    lane = lax.broadcasted_iota(jnp.int32, (2 * PFT_PAD, LANES), 1)
    mid = jnp.where(lane < LANES - ROWS, pltpu.roll(first, LANES - ROWS, 1), pltpu.roll(second, LANES - ROWS, 1))
    last = pltpu.roll(second, 2 * LANES - 2 * ROWS, 1)
    table = (first + mid + last) * scale
    own[...] = pack(table[:PFT_PAD])
    nxt[...] = pack(table[PFT_PAD:])

    @pl.when((x == 1) & (z == zs - 1))
    def _():
        gathered[pl.ds(pl.multiple_of((REGION + gx) * MAIN, 8), MAIN), :] = nxt[...]


    pl.semaphore_wait(barrier, len(partners))
    def chunk(s):
        return gathered.at[pl.ds(pl.multiple_of(s * MAIN, 8), MAIN), :]

    swap = pltpu.make_async_remote_copy(
        src_ref=own, dst_ref=theirs, send_sem=halo_send.at[0], recv_sem=halo_recv.at[0],
        device_id=dev_x, device_id_type=MESH,
    )
    shift = pltpu.make_async_remote_copy(
        src_ref=nxt, dst_ref=halo, send_sem=halo_send.at[1], recv_sem=halo_recv.at[1],
        device_id=dev(y, c, lax.rem(z + 1, zs), x), device_id_type=MESH,
    )
    shifts = (x == 1) & (z < zs - 1)
    shifted = (x == 1) & (z > 0)
    swap.start()

    @pl.when(shifts)
    def _():
        shift.start()

    swap.wait_recv()
    mine = pl.ds(pl.multiple_of(slot(y, c, z, x) * MAIN, 8), MAIN)

    @pl.when(x == 0)
    def _():
        gathered[mine, :] = theirs[...] + nxt[...]

    @pl.when((x == 1) & (z == 0))
    def _():
        gathered[mine, :] = theirs[...]

    @pl.when(shifted)
    def _():
        shift.wait_recv()
        gathered[mine, :] = theirs[...] + halo[...]

    sent = []

    def copy_of(s, target, sem):
        return pltpu.make_async_remote_copy(
            src_ref=chunk(s), dst_ref=chunk(s), send_sem=send_sem.at[sem],
            recv_sem=recv_sem.at[s], device_id=target, device_id_type=MESH,
        )

    def relay(owner, targets, arrives=True):
        y_, c_, z_, x_ = owner
        s, e = slot(y_, c_, z_, x_), REGION + y_ * 2 + c_
        edge = (z_ == zs - 1) & (x_ == 1)
        sems = [len(sent) + k for k in range(len(targets))]
        if arrives:
            copy_of(s, dev_x, 0).wait_recv()
        for target, sem in zip(targets, sems):
            copy_of(s, target, 2 * sem).start()

        @pl.when(edge)
        def _():
            if arrives:
                copy_of(e, dev_x, 0).wait_recv()
            for target, sem in zip(targets, sems):
                copy_of(e, target, 2 * sem + 1).start()

        sent.extend((s, e, edge, target, sem) for target, sem in zip(targets, sems))

    quad = [dev_d, dev_x, dev_y]
    relay((y, c, z, x), [dev(y, c, q, x) for q in line[:0:-1]] + quad + [dev_c], False)
    for q in line[1:]:
        relay((y, c, q, x), quad + [dev_c])
    for q in line:
        for y_, x_ in ((y, 1 - x), (1 - y, x), (1 - y, 1 - x)):
            relay((y_, c, q, x_), [dev_c])
    for q in line:
        for y_, x_ in ((y, x), (y, 1 - x), (1 - y, x), (1 - y, 1 - x)):
            relay((y_, 1 - c, q, x_), [])
    swap.wait_send()

    @pl.when(shifts)
    def _():
        shift.wait_send()

    for s, e, edge, target, sem in sent:
        copy_of(s, target, 2 * sem).wait_send()

        @pl.when(edge)
        def _(e=e, target=target, sem=sem):
            copy_of(e, target, 2 * sem + 1).wait_send()

    for g in range(2 * ys):
        first_row = pl.ds(((g + 1) % (2 * ys)) * ny * MAIN, MAIN)
        gathered[first_row, :] = gathered[first_row, :] + gathered[pl.ds((REGION + g) * MAIN, MAIN), :]

    for u in range(MAIN // 4):
        rows = [gathered[pl.ds(4 * u + j, REGION, stride=MAIN), :] for j in range(4)]
        tile = jnp.concatenate(rows, axis=0).T
        here = pl.ds(u * LANES, LANES)
        stored_ref[:, here] = tile[:POOLS]
        error_ref[:, here] = tile[POOLS:ROWS]
        if 4 * u < 2 * REST:
            t = (MAIN // 4) + (u if 4 * u < REST else u - REST // 4)
            w = min(LANES, CELLS - t * LANES)
            there = pl.ds(t * LANES, w)
            if 4 * u < REST:
                stored_ref[:, there] = tile[ROWS : ROWS + POOLS, :w]
                error_ref[: SPARE - POOLS, there] = tile[ROWS + POOLS :, :w]
            else:
                error_ref[SPARE - POOLS :, there] = tile[ROWS : 2 * ROWS - SPARE, :w]


def kernel_shards(zs, ys, pool_old, pool_new, flux, area, pft_id, region_id):
    patches = area.shape[0]
    devices = 4 * ys * zs
    scale = CELLS / (patches * devices)
    out = jax.ShapeDtypeStruct((POOLS, CELLS), jnp.float32)
    hbm, vmem = pl.BlockSpec(memory_space=pl.ANY), pl.BlockSpec(memory_space=pltpu.VMEM)
    sends = zs - 1 + 4 * zs + 3 * zs
    return pl.pallas_call(
        functools.partial(kernel, zs, ys, scale),
        out_shape=(out, out),
        in_specs=[hbm] * 3 + [vmem] * 3,
        out_specs=(vmem, vmem),
        scratch_shapes=[
            pltpu.VMEM((POOLS, patches), jnp.float32),
            pltpu.VMEM((POOLS, patches), jnp.float32),
            pltpu.VMEM((POOLS, patches), jnp.float32),
            pltpu.VMEM((MAIN, LANES), jnp.float32),
            pltpu.VMEM((MAIN, LANES), jnp.float32),
            pltpu.VMEM((MAIN, LANES), jnp.float32),
            pltpu.VMEM((MAIN, LANES), jnp.float32),
            pltpu.VMEM(((REGION + 2 * ys) * MAIN, LANES), jnp.float32),
            pltpu.SemaphoreType.DMA((3, BLOCKS)),
            pltpu.SemaphoreType.DMA((2,)),
            pltpu.SemaphoreType.DMA((2,)),
            pltpu.SemaphoreType.DMA((2 * sends,)),
            pltpu.SemaphoreType.DMA((devices + 2 * ys,)),
        ],
        compiler_params=pltpu.CompilerParams(collective_id=0, has_side_effects=True),
    )(pool_old, pool_new, flux, area[None, :], pft_id[None, :], region_id[None, :])


def shards(pool_old, pool_new, flux, area, pft_id, region_id):
    width_x = lax.axis_size("gx")
    width_y = lax.axis_size("gy")
    devices_all = width_x * width_y
    position = lax.axis_index("gx") * width_y + lax.axis_index("gy")
    base = position * REGION // devices_all
    offset_here = (region_id - base) % REGION
    compact_cell = pft_id * 2 + offset_here
    stored = area[None, :] * pool_new
    balance = area[None, :] * (pool_new - pool_old - 0.5 * flux)
    stacked = jnp.concatenate([stored, balance], axis=0)
    rows = stacked.shape[0]
    patch_count = stacked.shape[1]
    block = min(512, patch_count)
    blocks = patch_count // block
    stacked_blocks = stacked.reshape(rows, blocks, block).transpose(1, 0, 2)
    cell_blocks = compact_cell.reshape(blocks, block)
    columns = jnp.arange(2 * PFT, dtype=jnp.int32)

    def accumulate(totals, inputs):
        values, cells_here = inputs
        onehot = (cells_here[:, None] == columns[None, :]).astype(jnp.float32)
        added = jnp.dot(
            values, onehot, preferred_element_type=jnp.float32, precision=lax.Precision.HIGHEST
        )
        return (totals + added, None)

    local_table, _ = lax.scan(
        accumulate, jnp.zeros((rows, 2 * PFT), jnp.float32), (stacked_blocks, cell_blocks)
    )
    local_table = local_table.reshape(rows, PFT, 2)
    region_axis = jnp.arange(REGION, dtype=jnp.int32)
    pair_axis = jnp.arange(2, dtype=jnp.int32)
    span = REGION // width_x + 1
    start = lax.axis_index("gx") * (REGION // width_x)
    span_axis = jnp.arange(span, dtype=jnp.int32)
    into_group = ((base - start + pair_axis)[:, None] == span_axis[None, :]).astype(jnp.float32)
    group_table = jnp.einsum(
        "apj,jw->apw", local_table, into_group, precision=lax.Precision.HIGHEST
    )
    group_total = lax.psum(group_table, "gy")
    into_full = (((start + span_axis) % REGION)[:, None] == region_axis[None, :]).astype(
        jnp.float32
    )
    placed = jnp.einsum("apw,wr->apr", group_total, into_full, precision=lax.Precision.HIGHEST)
    totals = lax.psum(placed.reshape(rows, CELLS), "gx")
    patch_all = patch_count * devices_all
    totals = totals * jnp.float32(CELLS / patch_all)
    return (totals[:POOLS], totals[POOLS:])


def solution(mesh):
    wide, deep = mesh.shape["gx"], mesh.shape["gy"]
    if wide == 4 and wide * deep == REGION:
        local = functools.partial(kernel_shards, deep // 2, wide // 2)
    else:
        local = shards
    return jax.shard_map(
        local,
        mesh=mesh,
        in_specs=(
            P(None, ("gx", "gy")),
            P(None, ("gx", "gy")),
            P(None, ("gx", "gy")),
            P(("gx", "gy")),
            P(("gx", "gy")),
            P(("gx", "gy")),
        ),
        out_specs=(P(), P()),
        check_vma=False,
    )
```

```python
import functools
import jax
import jax.numpy as jnp
from jax import lax
from jax.experimental import pallas as pl
from jax.experimental.pallas import tpu as pltpu
from jax.sharding import PartitionSpec as P

POOLS = 40
PFT = 79
REGION = 32
CELLS = 2528
MESH = pl.DeviceIdType.MESH
ROWS = 2 * POOLS
PFT_PAD = 80
MAIN = 56
REST = PFT_PAD - MAIN
LANES = 128
SPARE = LANES - ROWS
BLOCKS = 4


def pack(table):
    main = table[:MAIN]
    rest = table[MAIN:]
    lane = lax.broadcasted_iota(jnp.int32, (REST, LANES), 1)
    first = pltpu.roll(rest, ROWS, 1)
    second = pltpu.roll(rest, ROWS - SPARE, 1)
    top = jnp.where(lane < ROWS, main[:REST], first)
    middle = jnp.where(lane < ROWS, main[REST : 2 * REST], second)
    return jnp.concatenate([top, middle, main[2 * REST :]], axis=0)


def kernel(
    zs, ys, scale,
    old_hbm, new_hbm, flux_hbm, area_ref, pft_ref, region_ref,
    out_ref,
    old_v, new_v, flux_v, own, nxt, theirs, halo, gathered,
    in_sem, halo_send, halo_recv, send_sem, recv_sem,
):
    gx, gy = lax.axis_index("gx"), lax.axis_index("gy")
    ny = 2 * zs
    devices = 2 * ys * ny
    patches = area_ref.shape[1]
    width = patches // BLOCKS
    y, c = gx // 2, gx % 2
    z, x = gy // 2, gy % 2
    me = gx * ny + gy
    copies = []
    for k in range(BLOCKS):
        part = pl.ds(k * width, width)
        for a, (src, dst) in enumerate(((new_hbm, new_v), (old_hbm, old_v), (flux_hbm, flux_v))):
            copy = pltpu.make_async_copy(src.at[:, part], dst.at[:, part], in_sem.at[a, k])
            copy.start()
            copies.append(copy)

    def dev(y_, c_, z_, x_):
        return (y_ * 2 + c_, z_ * 2 + x_)

    def slot(y_, c_, z_, x_):
        return (y_ * 2 + c_) * ny + z_ * 2 + 1 - x_

    by_distance = [sorted(range(zs), key=lambda q, a=a: (abs(q - a), q)) for a in range(zs)]
    line = [sum(jnp.where(z == a, by_distance[a][k], 0) for a in range(zs)) for k in range(zs)]
    dev_x, dev_y, dev_c = dev(y, c, z, 1 - x), dev(1 - y, c, z, x), dev(y, 1 - c, z, x)
    dev_d = dev(1 - y, c, z, 1 - x)
    partners = [dev(y, c, q, x) for q in line[1:]] + [dev_x, dev_y, dev_d, dev_c]
    barrier = pltpu.get_barrier_semaphore()
    for partner in partners:
        pl.semaphore_signal(barrier, inc=1, device_id=partner, device_id_type=MESH)

    base = me * REGION // devices
    total = None
    for k in range(BLOCKS):
        part = pl.ds(k * width, width)
        code = pft_ref[:, part] + jnp.where(region_ref[:, part] == base, 0, PFT_PAD)
        cells = lax.broadcasted_iota(jnp.int32, (2 * PFT_PAD, width), 0)
        hot = jnp.where(cells == code, 1.0, 0.0).astype(jnp.bfloat16)
        for copy in copies[3 * k : 3 * k + 3]:
            copy.wait()
        area = area_ref[:, part]
        new = new_v[:, part]
        stored = area * new
        balance = area * (new - old_v[:, part] - 0.5 * flux_v[:, part])
        values = jnp.concatenate([stored, balance], axis=0)
        high = values.astype(jnp.bfloat16)
        left = values - high.astype(jnp.float32)
        middle = left.astype(jnp.bfloat16)
        low = (left - middle.astype(jnp.float32)).astype(jnp.bfloat16)
        pieces = jnp.concatenate([high, middle, low], axis=0)
        added = lax.dot_general(hot, pieces, (((1,), (1,)), ((), ())), preferred_element_type=jnp.float32)
        total = added if total is None else total + added
    wide = jnp.concatenate([total, jnp.zeros((2 * PFT_PAD, 2 * LANES - 3 * ROWS), jnp.float32)], axis=1)
    first = wide[:, :LANES]
    second = wide[:, LANES:]
    lane = lax.broadcasted_iota(jnp.int32, (2 * PFT_PAD, LANES), 1)
    mid = jnp.where(lane < LANES - ROWS, pltpu.roll(first, LANES - ROWS, 1), pltpu.roll(second, LANES - ROWS, 1))
    last = pltpu.roll(second, 2 * LANES - 2 * ROWS, 1)
    table = (first + mid + last) * scale
    own[...] = pack(table[:PFT_PAD])
    nxt[...] = pack(table[PFT_PAD:])

    @pl.when((x == 1) & (z == zs - 1))
    def _():
        gathered[pl.ds(pl.multiple_of((REGION + gx) * MAIN, 8), MAIN), :] = nxt[...]


    pl.semaphore_wait(barrier, len(partners))
    def chunk(s):
        return gathered.at[pl.ds(pl.multiple_of(s * MAIN, 8), MAIN), :]

    swap = pltpu.make_async_remote_copy(
        src_ref=own, dst_ref=theirs, send_sem=halo_send.at[0], recv_sem=halo_recv.at[0],
        device_id=dev_x, device_id_type=MESH,
    )
    shift = pltpu.make_async_remote_copy(
        src_ref=nxt, dst_ref=halo, send_sem=halo_send.at[1], recv_sem=halo_recv.at[1],
        device_id=dev(y, c, lax.rem(z + 1, zs), x), device_id_type=MESH,
    )
    shifts = (x == 1) & (z < zs - 1)
    shifted = (x == 1) & (z > 0)
    swap.start()

    @pl.when(shifts)
    def _():
        shift.start()

    swap.wait_recv()
    mine = pl.ds(pl.multiple_of(slot(y, c, z, x) * MAIN, 8), MAIN)

    @pl.when(x == 0)
    def _():
        gathered[mine, :] = theirs[...] + nxt[...]

    @pl.when((x == 1) & (z == 0))
    def _():
        gathered[mine, :] = theirs[...]

    @pl.when(shifted)
    def _():
        shift.wait_recv()
        gathered[mine, :] = theirs[...] + halo[...]

    sent = []

    def copy_of(s, target, sem):
        return pltpu.make_async_remote_copy(
            src_ref=chunk(s), dst_ref=chunk(s), send_sem=send_sem.at[sem],
            recv_sem=recv_sem.at[s], device_id=target, device_id_type=MESH,
        )

    def relay(owner, targets, arrives=True):
        y_, c_, z_, x_ = owner
        s, e = slot(y_, c_, z_, x_), REGION + y_ * 2 + c_
        edge = (z_ == zs - 1) & (x_ == 1)
        sems = [len(sent) + k for k in range(len(targets))]
        if arrives:
            copy_of(s, dev_x, 0).wait_recv()
        for target, sem in zip(targets, sems):
            copy_of(s, target, 2 * sem).start()

        @pl.when(edge)
        def _():
            if arrives:
                copy_of(e, dev_x, 0).wait_recv()
            for target, sem in zip(targets, sems):
                copy_of(e, target, 2 * sem + 1).start()

        sent.extend((s, e, edge, target, sem) for target, sem in zip(targets, sems))

    quad = [dev_d, dev_x, dev_y]
    relay((y, c, z, x), [dev(y, c, q, x) for q in line[:0:-1]] + quad + [dev_c], False)
    for q in line[1:]:
        relay((y, c, q, x), quad + [dev_c])
    for q in line:
        for y_, x_ in ((y, 1 - x), (1 - y, x), (1 - y, 1 - x)):
            relay((y_, c, q, x_), [dev_c])
    for q in line:
        for y_, x_ in ((y, x), (y, 1 - x), (1 - y, x), (1 - y, 1 - x)):
            relay((y_, 1 - c, q, x_), [])
    swap.wait_send()

    @pl.when(shifts)
    def _():
        shift.wait_send()

    for s, e, edge, target, sem in sent:
        copy_of(s, target, 2 * sem).wait_send()

        @pl.when(edge)
        def _(e=e, target=target, sem=sem):
            copy_of(e, target, 2 * sem + 1).wait_send()

    for g in range(2 * ys):
        first_row = pl.ds(((g + 1) % (2 * ys)) * ny * MAIN, MAIN)
        gathered[first_row, :] = gathered[first_row, :] + gathered[pl.ds((REGION + g) * MAIN, MAIN), :]

    for u in range(MAIN // 4):
        rows = [gathered[pl.ds(4 * u + j, REGION, stride=MAIN), :] for j in range(4)]
        tile = jnp.concatenate(rows, axis=0).T
        here = pl.ds(u * LANES, LANES)
        out_ref[:, here] = tile[:ROWS]
        if 4 * u < 2 * REST:
            t = (MAIN // 4) + (u if 4 * u < REST else u - REST // 4)
            w = min(LANES, CELLS - t * LANES)
            there = pl.ds(t * LANES, w)
            if 4 * u < REST:
                out_ref[:SPARE, there] = tile[ROWS:, :w]
            else:
                out_ref[SPARE:, there] = tile[ROWS : 2 * ROWS - SPARE, :w]


def kernel_shards(zs, ys, pool_old, pool_new, flux, area, pft_id, region_id):
    patches = area.shape[0]
    devices = 4 * ys * zs
    scale = CELLS / (patches * devices)
    out = jax.ShapeDtypeStruct((ROWS, CELLS), jnp.float32)
    hbm, vmem = pl.BlockSpec(memory_space=pl.ANY), pl.BlockSpec(memory_space=pltpu.VMEM)
    sends = zs - 1 + 4 * zs + 3 * zs
    both = pl.pallas_call(
        functools.partial(kernel, zs, ys, scale),
        out_shape=out,
        in_specs=[hbm] * 3 + [vmem] * 3,
        out_specs=vmem,
        scratch_shapes=[
            pltpu.VMEM((POOLS, patches), jnp.float32),
            pltpu.VMEM((POOLS, patches), jnp.float32),
            pltpu.VMEM((POOLS, patches), jnp.float32),
            pltpu.VMEM((MAIN, LANES), jnp.float32),
            pltpu.VMEM((MAIN, LANES), jnp.float32),
            pltpu.VMEM((MAIN, LANES), jnp.float32),
            pltpu.VMEM((MAIN, LANES), jnp.float32),
            pltpu.VMEM(((REGION + 2 * ys) * MAIN, LANES), jnp.float32),
            pltpu.SemaphoreType.DMA((3, BLOCKS)),
            pltpu.SemaphoreType.DMA((2,)),
            pltpu.SemaphoreType.DMA((2,)),
            pltpu.SemaphoreType.DMA((2 * sends,)),
            pltpu.SemaphoreType.DMA((devices + 2 * ys,)),
        ],
        compiler_params=pltpu.CompilerParams(collective_id=0, has_side_effects=True),
    )(pool_old, pool_new, flux, area[None, :], pft_id[None, :], region_id[None, :])
    return (both[:POOLS], both[POOLS:])


def shards(pool_old, pool_new, flux, area, pft_id, region_id):
    width_x = lax.axis_size("gx")
    width_y = lax.axis_size("gy")
    devices_all = width_x * width_y
    position = lax.axis_index("gx") * width_y + lax.axis_index("gy")
    base = position * REGION // devices_all
    offset_here = (region_id - base) % REGION
    compact_cell = pft_id * 2 + offset_here
    stored = area[None, :] * pool_new
    balance = area[None, :] * (pool_new - pool_old - 0.5 * flux)
    stacked = jnp.concatenate([stored, balance], axis=0)
    rows = stacked.shape[0]
    patch_count = stacked.shape[1]
    block = min(512, patch_count)
    blocks = patch_count // block
    stacked_blocks = stacked.reshape(rows, blocks, block).transpose(1, 0, 2)
    cell_blocks = compact_cell.reshape(blocks, block)
    columns = jnp.arange(2 * PFT, dtype=jnp.int32)

    def accumulate(totals, inputs):
        values, cells_here = inputs
        onehot = (cells_here[:, None] == columns[None, :]).astype(jnp.float32)
        added = jnp.dot(
            values, onehot, preferred_element_type=jnp.float32, precision=lax.Precision.HIGHEST
        )
        return (totals + added, None)

    local_table, _ = lax.scan(
        accumulate, jnp.zeros((rows, 2 * PFT), jnp.float32), (stacked_blocks, cell_blocks)
    )
    local_table = local_table.reshape(rows, PFT, 2)
    region_axis = jnp.arange(REGION, dtype=jnp.int32)
    pair_axis = jnp.arange(2, dtype=jnp.int32)
    span = REGION // width_x + 1
    start = lax.axis_index("gx") * (REGION // width_x)
    span_axis = jnp.arange(span, dtype=jnp.int32)
    into_group = ((base - start + pair_axis)[:, None] == span_axis[None, :]).astype(jnp.float32)
    group_table = jnp.einsum(
        "apj,jw->apw", local_table, into_group, precision=lax.Precision.HIGHEST
    )
    group_total = lax.psum(group_table, "gy")
    into_full = (((start + span_axis) % REGION)[:, None] == region_axis[None, :]).astype(
        jnp.float32
    )
    placed = jnp.einsum("apw,wr->apr", group_total, into_full, precision=lax.Precision.HIGHEST)
    totals = lax.psum(placed.reshape(rows, CELLS), "gx")
    patch_all = patch_count * devices_all
    totals = totals * jnp.float32(CELLS / patch_all)
    return (totals[:POOLS], totals[POOLS:])


def solution(mesh):
    wide, deep = mesh.shape["gx"], mesh.shape["gy"]
    if wide == 4 and wide * deep == REGION:
        local = functools.partial(kernel_shards, deep // 2, wide // 2)
    else:
        local = shards
    return jax.shard_map(
        local,
        mesh=mesh,
        in_specs=(
            P(None, ("gx", "gy")),
            P(None, ("gx", "gy")),
            P(None, ("gx", "gy")),
            P(("gx", "gy")),
            P(("gx", "gy")),
            P(("gx", "gy")),
        ),
        out_specs=(P(), P()),
        check_vma=False,
    )
```
